32 devices in a mesh: gx: 8 (over y, x, core), gy: 4 (over z).
Axes of the slice: x: 2, y: 2, z: 4, core: 2. Of those that a mesh axis runs over, the one named last changes fastest.
Arguments:
- candidate_owner: int32 [256, 512, 1], P(('gx', 'gy')), may hold values from 0 to 31; in each aligned block of 4096 rows (0 to 4095, 4096 to 8191, ..., all dimensions but the last counted through in order) at most 256 rows name the same one
- candidate_row: int32 [256, 512], P(('gx', 'gy')), may hold values from 0 to 78335
- item_table: bfloat16 [2506752, 128], P(('gx', 'gy')), may hold values from -6 to 6
- w_in: bfloat16 [128, 512], replicated, may hold values from -0.5 to 0.5
- w_qkv: bfloat16 [1, 512, 1536], replicated, may hold values from -0.25 to 0.25
- w_out: bfloat16 [1, 512, 512], replicated, may hold values from -0.25 to 0.25
- w_up: bfloat16 [1, 512, 1024], replicated, may hold values from -0.25 to 0.25
- w_down: bfloat16 [1, 1024, 512], replicated, may hold values from -0.1875 to 0.1875
- norm_gains: float32 [1, 2, 512], replicated, may hold values from 0.25 to 1.75
- final_gain: float32 [512], replicated, may hold values from 0.25 to 1.75
- w_score: bfloat16 [512], replicated, may hold values from -0.25 to 0.25
Outputs:
- log_probs: float32 [256, 512], P(('gx', 'gy'))
The draws below stay inside these ranges and needn't reach their ends.
Inputs may be any that keep to these rules, and one draw needn't show every extreme that they name: `candidate_owner`: among the candidates of one device's 8 slates no shard is named more than 256 times, a bound that some block reaches.
All inputs are finite; a program needn't handle non-finite values.
Results may differ from the reference program's by a relative error of at most 0.0007.
Values may be sent and summed in bfloat16 or wider, within the bound.
A program may use at most 128 MiB of HBM per device.

```python
import math
import jax
import jax.numpy as jnp
import numpy as np
from jax import lax

SLATE_LEN = 512
SLATES_DEV = 8
SLATES = 256
EMB = 128
ROWS_DEV = 78336
ROWS = 2506752
D = 512
HEADS = 8
FF = 1024
LAYERS = 1
CAP = 256
N_GX = 8
N_GY = 4


def set_ends(values, rng, smallest, largest):
    dims = values.shape
    place = [jax.random.randint(jax.random.fold_in(rng, axis), (), 0, dims[axis]) for axis in range(len(dims))]
    values = values.at[tuple(place)].set(smallest)
    longest = dims.index(max(dims))
    place[longest] = (place[longest] + 1) % dims[longest]
    return values.at[tuple(place)].set(largest)


def shard_levels(stream_key, shape, split, smallest, high):
    level, own = 1.0, jax.random.fold_in(stream_key, 6)
    for position, shards_of in split:
        steps = jnp.exp(jax.random.uniform(jax.random.fold_in(own, position), (shards_of,), jnp.float32, smallest / len(split), high / len(split)))
        level = level * jnp.repeat(steps, shape[position] // shards_of).reshape([-1 if axis == position else 1 for axis in range(len(shape))])
    return level


def wide_ids(key, dims, number_of, slope):
    portions = [min(1 << octave, number_of + 1 - (1 << octave)) * (1 << 20) // math.isqrt((1 << octave) ** slope) + 1 for octave in range((number_of + 1).bit_length()) if 1 << octave <= number_of]
    spread = 1 + sum(portions) // (1 << 30)
    listing = np.cumsum(np.array([max(1, weight // spread) for weight in portions]))
    pick = jax.random.randint(jax.random.fold_in(key, 1), dims, 0, int(listing[len(portions) - 1]))
    start = jnp.left_shift(1, jnp.searchsorted(jnp.asarray(listing, jnp.int32), pick, side="right").astype(jnp.int32))
    grade = start - 1 + jax.random.randint(jax.random.fold_in(key, 4), dims, 0, 1 << 30) % jnp.minimum(start, number_of + 1 - start)
    return jax.random.permutation(jax.random.fold_in(key, 2), number_of)[grade].astype(jnp.int32)


def deal_out(rng, own, number, rows, number_of, top, bound, skew):
    sequence = jax.random.permutation(rng, number_of)
    packed, common = load_shares(number_of, rows * top, bound, skew, True), load_shares(number_of, rows * top, bound, skew, False)
    places = jnp.arange(number_of)

    def named(lengths, turn):
        used = int((lengths > 0).sum())
        fixed = max(1, used // 4)
        moved = fixed + (places - fixed + turn * (used - fixed)) % max(1, number_of - fixed)
        return jnp.zeros((number_of,), jnp.int32).at[sequence[jnp.where(places < fixed, places, moved)]].set(jnp.asarray(lengths, jnp.int32))

    lengths = jnp.where(number % 4 == 0, named(packed, number // 4), named(common, number - number // 4 - 1))
    mixed = jax.random.permutation(jax.random.fold_in(own, 3), number_of)
    source_of, sink = mixed[0:number_of // 2 * 2:2], mixed[1:number_of // 2 * 2:2]
    room = jnp.minimum(lengths[source_of] - 1, bound - lengths[sink]) // 2
    room = jnp.where((source_of == sequence[0]) | (sink == sequence[0]) | (lengths[sink] == 0), 0, jnp.maximum(room, 0))
    moved = jax.random.randint(jax.random.fold_in(own, 4), (number_of // 2,), 0, 1 << 20) % (room + 1)
    lengths = lengths.at[source_of].add(-moved).at[sink].add(moved)
    members = jnp.searchsorted(jnp.cumsum(lengths), jnp.arange(rows * top), side="right").astype(jnp.int32)
    grid = members.reshape(top, rows).T
    grid = grid[jax.random.permutation(jax.random.fold_in(own, 1), rows)]
    turn = jax.random.randint(jax.random.fold_in(own, 2), (rows, 1), 0, top)
    return jnp.take_along_axis(grid, (jnp.arange(top)[None, :] + turn) % top, axis=1)


def load_shares(amount, total, limit, lean, full):
    portions = [(1 << 20) // math.isqrt(standing ** lean) + 1 for standing in range(1, amount + 1)]
    largest = limit if full else min(limit, max(-(-total // amount), total * portions[0] // sum(portions)))
    least = 1 if total - largest >= amount - 1 else 0
    holding, rest = [largest] + [least] * (amount - 1), total - largest - least * (amount - 1)
    while rest > 0:
        free = [i for i in range(1, amount) if holding[i] < largest] or [i for i in range(1, amount) if holding[i] < limit]
        pool, budget = sum([portions[i] for i in free]), rest
        for i in free:
            addition = min(limit - holding[i], max(1, budget * portions[i] // pool), rest)
            holding[i] = holding[i] + addition
            rest = rest - addition
    return np.array(holding)


def normal_values(own_key, extent, scale, most, pieces=(), dtype=jnp.bfloat16):
    factor_of = shard_levels(own_key, extent, pieces, -0.22, 0.18) if pieces else 1.0
    drawn = jax.random.normal(own_key, extent, jnp.float32) * scale * factor_of
    return jnp.minimum(jnp.maximum(drawn, -most), most).astype(dtype)


def setup_inputs(seed: int = 0) -> dict:
    arg_keys = jax.random.split(jax.random.key(seed), 12)
    candidate_owner_keys = jax.random.split(jax.random.fold_in(arg_keys[0], 1), SLATES * SLATE_LEN // (SLATES_DEV * SLATE_LEN))
    candidate_owner_turns = jax.random.permutation(jax.random.fold_in(arg_keys[0], 3), SLATES * SLATE_LEN // (SLATES_DEV * SLATE_LEN))
    candidate_owner = jax.vmap(lambda own, number: deal_out(jax.random.fold_in(arg_keys[0], 2), own, number, SLATES_DEV * SLATE_LEN, N_GX * N_GY, 1, CAP, 2))(candidate_owner_keys, candidate_owner_turns).reshape((SLATES, SLATE_LEN, 1))
    candidate_row = set_ends(wide_ids(arg_keys[1], (SLATES, SLATE_LEN), ROWS_DEV, 2), jax.random.fold_in(arg_keys[1], 3), 0, ROWS_DEV - 1).astype(jnp.int32)
    item_table = normal_values(arg_keys[2], (ROWS, EMB), 1.0, 6.0, ((0, 32),))
    w_in = normal_values(arg_keys[3], (EMB, D), EMB ** -0.5, 0.5)
    w_qkv = normal_values(arg_keys[4], (LAYERS, D, 3 * D), D ** -0.5, 0.25)
    w_out = normal_values(arg_keys[5], (LAYERS, D, D), D ** -0.5, 0.25)
    w_up = normal_values(arg_keys[6], (LAYERS, D, FF), D ** -0.5, 0.25)
    w_down = normal_values(arg_keys[7], (LAYERS, FF, D), FF ** -0.5, 0.1875)
    norm_gains = jnp.clip(1.0 + 0.15 * jax.random.normal(arg_keys[8], (LAYERS, 2, D), jnp.float32), 0.25, 1.75)
    final_gain = jnp.clip(1.0 + 0.15 * jax.random.normal(arg_keys[9], (D,), jnp.float32), 0.25, 1.75)
    w_score = normal_values(arg_keys[10], (D,), D ** -0.5, 0.25)
    return dict(candidate_owner=candidate_owner, candidate_row=candidate_row, item_table=item_table, w_in=w_in, w_qkv=w_qkv, w_out=w_out, w_up=w_up, w_down=w_down, norm_gains=norm_gains, final_gain=final_gain, w_score=w_score)


def layer_norm(values, gain):
    mean = lax.optimization_barrier(jnp.mean(values, axis=-1, keepdims=True))
    centred = values - mean
    variance = lax.optimization_barrier(jnp.mean(centred * centred, axis=-1, keepdims=True))
    return centred * lax.rsqrt(variance + 1e-05) * gain

def score_slates(emb, w_in, w_qkv, w_out, w_up, w_down, norm_gains, final_gain, w_score):
    slates, length, width = emb.shape
    model = w_in.shape[1]
    head_dim = model // HEADS
    resid = jnp.dot(emb.reshape(slates * length, width), w_in, preferred_element_type=jnp.float32)
    for layer in range(LAYERS):
        normed = layer_norm(resid, norm_gains[layer, 0]).astype(jnp.bfloat16)
        qkv = jnp.dot(normed, w_qkv[layer], preferred_element_type=jnp.float32).astype(jnp.bfloat16)
        qkv = qkv.reshape(slates, length, 3, HEADS, head_dim)
        query = qkv[:, :, 0].astype(jnp.float32)
        keys = qkv[:, :, 1].astype(jnp.float32)
        values = qkv[:, :, 2].astype(jnp.float32)
        scores = jnp.einsum('bqhd,bkhd->bhqk', query, keys) * head_dim ** (-0.5)
        probs = jax.nn.softmax(scores, axis=-1).astype(jnp.bfloat16)
        mixed = jnp.einsum('bhqk,bkhd->bqhd', probs.astype(jnp.float32), values)
        mixed = mixed.astype(jnp.bfloat16).reshape(slates * length, model)
        resid = resid + jnp.dot(mixed, w_out[layer], preferred_element_type=jnp.float32)
        normed = layer_norm(resid, norm_gains[layer, 1]).astype(jnp.bfloat16)
        inner = jax.nn.gelu(jnp.dot(normed, w_up[layer], preferred_element_type=jnp.float32)).astype(jnp.bfloat16)
        resid = resid + jnp.dot(inner, w_down[layer], preferred_element_type=jnp.float32)
    final = layer_norm(resid, final_gain)
    logits = lax.optimization_barrier(jnp.sum(final * w_score.astype(jnp.float32)[None, :], axis=-1))
    return jax.nn.log_softmax(logits.reshape(slates, length), axis=-1)

def reference(candidate_owner, candidate_row, item_table, w_in, w_qkv, w_out, w_up, w_down, norm_gains, final_gain, w_score):
    item = (candidate_owner[:, :, 0] * ROWS_DEV + candidate_row).astype(jnp.int32)
    emb = jnp.take(item_table, item.reshape(-1), axis=0)
    emb = emb.reshape(N_GX * N_GY * SLATES_DEV, 1, SLATE_LEN, EMB)

    def one_group(block):
        return score_slates(block, w_in, w_qkv, w_out, w_up, w_down, norm_gains, final_gain, w_score)
    scored = lax.map(one_group, emb)
    return scored.reshape(SLATES, SLATE_LEN)
```

```python
import functools
import math
import jax
import jax.numpy as jnp
from jax import lax
from jax.experimental import pallas as pl
from jax.experimental.pallas import tpu as pltpu
from jax.sharding import PartitionSpec as P

HEADS = 8
PICK = 32
BUFFERS = 3
EARLY = 5
LOG2E = 1.4426950408889634
LIMIT = 2.0**60
f32, bf16, i32 = jnp.float32, jnp.bfloat16, jnp.int32
MESH = pl.DeviceIdType.MESH


def chunk_ends(capacity):
    return sorted({-(-capacity * part // 128) * 16 for part in (2, 4, 5, 6, 7, 8)})


def ready_chunks(capacity, slates):
    ends, ready = chunk_ends(capacity), []
    for slate in range(slates):
        part = (slate + 1) / slates
        need = min(capacity, capacity * part + 4 * math.sqrt(capacity * part * (1 - part) * (1 - 1 / 16)))
        ready.append(next(chunk for chunk, end in enumerate(ends) if end >= need))
    return ready


def block_size(rows):
    return next(size for size in range(4608, 0, -16) if rows % size == 0)


def norm_cols(values, gain):
    scale = 1.0 / values.shape[0]
    mean = jnp.sum(values, axis=0, keepdims=True) * scale
    centred = values - mean
    variance = jnp.sum(centred * centred, axis=0, keepdims=True) * scale
    return centred * lax.rsqrt(variance + 1e-05) * gain


def score_slate(emb, weights, gain_of, scratch, exact):
    w_in, w_qkv, w_out, w_up, w_down = weights
    resid_ref, query_ref, keys_ref, value_ref, mixed_ref = scratch
    model, length = w_in.shape[0], emb.shape[0]
    head_dim = model // HEADS
    pack = 128 // head_dim
    resid = lax.dot_general(w_in[...], emb, (((1,), (1,)), ((), ())), preferred_element_type=f32)
    resid_ref[...] = resid
    normed = norm_cols(resid, gain_of(0)).astype(bf16)
    keys_ref[...] = jnp.dot(w_qkv[model : 2 * model], normed, preferred_element_type=f32).astype(bf16).T
    query = jnp.dot(w_qkv[:model], normed, preferred_element_type=f32)
    query_ref[...] = (query * (LOG2E * head_dim ** (-0.5))).astype(bf16)
    value_ref[...] = jnp.dot(w_qkv[2 * model :], normed, preferred_element_type=f32).astype(bf16)
    zeros = jnp.zeros((head_dim, length), bf16)
    ones = jnp.ones((16, length), bf16)

    def scores_of(head):
        group, part = head // pack, head % pack
        query = query_ref[head * head_dim : (head + 1) * head_dim, :]
        query = jnp.concatenate([query if p == part else zeros for p in range(pack)], axis=0)
        return jnp.dot(keys_ref[:, group * 128 : (group + 1) * 128], query, preferred_element_type=f32)

    low = high = None
    ahead = scores_of(0)
    for head in range(HEADS):
        rows = slice(head * head_dim, (head + 1) * head_dim)
        scores = ahead
        if head + 1 < HEADS:
            ahead = scores_of(head + 1)
        if exact:
            scores = scores - jnp.max(scores, axis=0, keepdims=True)
        probs = jnp.exp2(scores).astype(bf16)
        stacked = jnp.concatenate([value_ref[rows, :], ones], axis=0)
        both = jnp.dot(stacked, probs, preferred_element_type=f32)
        total = both[head_dim : head_dim + 1]
        low = total if low is None else jnp.minimum(low, total)
        high = total if high is None else jnp.maximum(high, total)
        mixed_ref[rows, :] = (both[:head_dim] * (1.0 / total)).astype(bf16)
    resid = resid_ref[...] + jnp.dot(w_out[...], mixed_ref[...], preferred_element_type=f32)
    resid_ref[...] = resid
    normed = norm_cols(resid, gain_of(1)).astype(bf16)
    inner = jnp.dot(w_up[...], normed, preferred_element_type=f32)
    half = 0.5 * inner
    inner = half + half * jnp.tanh(inner * (0.7978845608028654 + 0.035677408136300125 * (inner * inner)))
    resid = resid_ref[...] + jnp.dot(w_down[...], inner.astype(bf16), preferred_element_type=f32)
    logits = jnp.sum(norm_cols(resid, gain_of(2)) * gain_of(3), axis=0, keepdims=True)
    shifted = logits - jnp.max(logits, axis=-1, keepdims=True)
    result = shifted - jnp.log(jnp.sum(jnp.exp(shifted), axis=-1, keepdims=True))
    return result, low, high


def score_scratch(model, length):
    return [
        pltpu.VMEM((model, length), f32),
        pltpu.VMEM((model, length), bf16),
        pltpu.VMEM((length, model), bf16),
        pltpu.VMEM((model, length), bf16),
        pltpu.VMEM((model, length), bf16),
    ]


def turn_weights(raw, turned):
    for source, target in zip(raw, turned):
        rows, cols = source.shape
        for row in range(0, rows, 512):
            for col in range(0, cols, 512):
                r, c = slice(row, min(rows, row + 512)), slice(col, min(cols, col + 512))
                target[c, r] = source[r, c].T


def spread_gains(gain_refs, target, base):
    norm_ref, final_ref, score_ref = gain_refs
    model = norm_ref.shape[1]
    gains = [norm_ref[...], final_ref[...], score_ref[...].astype(f32), jnp.zeros((4, model), f32)]
    columns = jnp.concatenate(gains, axis=0).T
    for row in range(4):
        target[base + row * model : base + (row + 1) * model, :] = jnp.broadcast_to(
            columns[:, row : row + 1], (model, 128)
        )


def widen(gains_ref, base, row, model, length):
    gain = gains_ref[base + row * model : base + (row + 1) * model, :]
    return jnp.concatenate([gain] * (length // 128), axis=1)


def route(owner_ref, row_ref, asks_ref, place_ref, capacity, shards, rows, bounds):
    slates, length = owner_ref.shape
    ends = chunk_ends(capacity)
    shard = lax.broadcasted_iota(i32, (shards, length), 0)
    slots = lax.broadcasted_iota(i32, (capacity, length), 0)
    upper = lax.broadcasted_iota(i32, (length, length), 0) <= lax.broadcasted_iota(i32, (length, length), 1)
    upper = upper.astype(f32).astype(bf16)
    hits = [(owner_ref[b : b + 1, :] == shard).astype(f32) for b in range(slates)]
    within = jnp.dot(jnp.concatenate(hits, axis=0).astype(bf16), upper, preferred_element_type=f32)
    before = jnp.zeros((shards, 1), f32)
    found, late = None, None
    for b in range(slates):
        counts = within[b * shards : (b + 1) * shards]
        slot = jnp.sum(hits[b] * (counts + before), axis=0, keepdims=True).astype(i32) - 1
        before = before + counts[:, length - 1 : length]
        owner, index = owner_ref[b : b + 1, :], row_ref[b : b + 1, :]
        place = owner * ends[0] + slot
        for start, end in zip(ends[:-1], ends[1:]):
            here = shards * start + owner * (end - start) + (slot - start)
            place = jnp.where(slot >= start, here, place)
        place_ref[b : b + 1, :] = jnp.clip(place, 0, shards * capacity - 1)
        over = (slot >= bounds[b]).astype(i32)
        late = over if late is None else jnp.maximum(late, over)
        at_slot = (slot == slots).astype(f32).astype(bf16)
        digits = (index >> 16, (index >> 8) & 255, index & 255)
        placed = jnp.concatenate([hits[b] * digit.astype(f32) for digit in digits], axis=0).astype(bf16)
        part = lax.dot_general(placed, at_slot, (((1,), (1,)), ((), ())), preferred_element_type=f32)
        found = part if found is None else found + part
    found = found.astype(i32)
    asks = (found[:shards] << 16) + (found[shards : 2 * shards] << 8) + found[2 * shards :]
    asks = jnp.clip(asks, 0, rows - 1)
    for peer in range(shards):
        asks_ref[peer] = asks[peer : peer + 1, :]
    return late


def rank_kernel(capacity, owner_ref, row_ref, norm_ref, final_ref, score_ref, table_ref, *refs):
    chunks = len(chunk_ends(capacity))
    raw_hbm, refs = refs[:5], refs[5:]
    out_ref, flag_ref, place_ref = refs[:3]
    kept_refs, refs = refs[3 : 3 + chunks], refs[3 + chunks :]
    rows_ref, stream_ref, asks_ref, wanted_ref, wanted_smem, place_smem, stage_ref, emb_ref, worst_ref = refs[:9]
    send_refs, refs = refs[9 : 9 + chunks], refs[9 + chunks :]
    recv_refs, refs = refs[:chunks], refs[chunks:]
    raw, turned, refs = refs[:5], refs[5:10], refs[10:]
    scratch, refs = refs[:5], refs[5:]
    (
        stream_sems, raw_sems, ask_send_sem, ask_recv_sem, smem_sems,
        send_sems, recv_sems, keep_sems,
    ) = refs
    inner = lax.axis_size("gy")
    count = lax.axis_size("gx") * inner
    here = lax.axis_index("gx") * inner + lax.axis_index("gy")
    slates, length = owner_ref.shape
    model = norm_ref.shape[1]
    ends = chunk_ends(capacity)
    starts = [0] + ends[:-1]
    ready = ready_chunks(capacity, slates)
    barrier = pltpu.get_barrier_semaphore()

    def peer_of(step):
        peer = lax.rem(here + step, count)
        return peer, (peer // inner, lax.rem(peer, inner))

    @pl.loop(1, count)
    def _(step):
        pl.semaphore_signal(barrier, inc=1, device_id=peer_of(step)[1], device_id_type=MESH)

    size = stream_ref.shape[1]
    blocks = table_ref.shape[0] // size

    def stream(block):
        slot = lax.rem(block, BUFFERS)
        return pltpu.make_async_copy(
            table_ref.at[pl.ds(pl.multiple_of(block * size, size), size)], stream_ref.at[slot], stream_sems.at[slot]
        )

    for block in range(min(BUFFERS, blocks)):
        stream(block).start()
    copies = [pltpu.make_async_copy(s, t, raw_sems.at[n]) for n, (s, t) in enumerate(zip(raw_hbm, raw))]
    for copy in copies:
        copy.start()

    def load(block):
        stream(block).wait()
        start = pl.multiple_of(block * size, size)
        rows_ref[pl.ds(start, size), :] = stream_ref[lax.rem(block, BUFFERS)].astype(f32)

        @pl.when(block + BUFFERS < blocks)
        def _():
            stream(block + BUFFERS).start()

    late = route(
        owner_ref, row_ref, asks_ref, place_ref, capacity, count, table_ref.shape[0], [ends[chunk] for chunk in ready]
    )
    place_copy = pltpu.make_async_copy(place_ref, place_smem, smem_sems.at[0])
    place_copy.start()

    early = min(EARLY, blocks)

    @pl.loop(0, early)
    def _(block):
        load(block)

    def ask(step):
        peer, device = peer_of(step)
        return pltpu.make_async_remote_copy(
            src_ref=asks_ref.at[peer],
            dst_ref=wanted_ref.at[here],
            send_sem=ask_send_sem,
            recv_sem=ask_recv_sem,
            device_id=device,
            device_id_type=MESH,
        )

    pl.semaphore_wait(barrier, count - 1)

    @pl.loop(1, count)
    def _(step):
        ask(step).start()

    wanted_ref[here] = asks_ref[here]

    @pl.loop(early, blocks)
    def _(block):
        load(block)

    others = pl.ds(0, count - 1)
    pltpu.make_async_copy(asks_ref.at[others], asks_ref.at[others], ask_send_sem).wait()
    pltpu.make_async_copy(wanted_ref.at[others], wanted_ref.at[others], ask_recv_sem).wait()
    wanted_copy = pltpu.make_async_copy(wanted_ref, wanted_smem, smem_sems.at[1])
    wanted_copy.start()
    wanted_copy.wait()

    def give(chunk, step):
        peer, device = peer_of(step)
        return pltpu.make_async_remote_copy(
            src_ref=send_refs[chunk].at[peer],
            dst_ref=recv_refs[chunk].at[here],
            send_sem=send_sems.at[chunk],
            recv_sem=recv_sems.at[chunk],
            device_id=device,
            device_id_type=MESH,
        )

    def pick(chunk, step):
        peer = peer_of(step)[0]
        depth = ends[chunk] - starts[chunk]
        for row in range(depth):
            index = wanted_smem[peer, 0, starts[chunk] + row]
            stage_ref[row : row + 1, :] = rows_ref[pl.ds(index, 1), :]
        send_refs[chunk][peer] = stage_ref[:depth, :].astype(bf16)

    for chunk in range(chunks):

        @pl.loop(1, count)
        def _(step):
            pick(chunk, step)
            give(chunk, step).start()

        pick(chunk, 0)

    place_copy.wait()
    for copy in copies:
        copy.wait()
    turn_weights(raw, turned)
    gains_base = count * capacity
    spread_gains((norm_ref, final_ref, score_ref), rows_ref, gains_base)

    def keep(chunk):
        return pltpu.make_async_copy(recv_refs[chunk], kept_refs[chunk], keep_sems.at[chunk])

    def take(chunk):
        depth, base = ends[chunk] - starts[chunk], count * starts[chunk]
        landed = recv_refs[chunk]
        pltpu.make_async_copy(landed.at[others], landed.at[others], recv_sems.at[chunk]).wait()
        landed[here] = send_refs[chunk][here]
        keep(chunk).start()

        @pl.loop(0, count)
        def _(peer):
            start = pl.multiple_of(base + peer * depth, 16)
            rows_ref[pl.ds(start, depth), :] = landed[peer].astype(f32)

    @pl.loop(0, slates)
    def _(slate):
        for chunk in range(chunks):
            first = next(s for s in range(slates) if ready[s] >= chunk)

            @pl.when(slate == first)
            def _():
                take(chunk)

        @pl.loop(0, length // PICK)
        def _(block):
            for row in range(PICK):
                index = block * PICK + row
                emb_ref[pl.ds(index, 1), :] = rows_ref[pl.ds(place_smem[slate, index], 1), :]

        gain_of = lambda row: widen(rows_ref, gains_base, row, model, length)
        result, low, high = score_slate(emb_ref[...].astype(bf16), turned, gain_of, scratch, False)
        out_ref[slate] = result
        bad = jnp.where((low > 1.0 / LIMIT) & (high < LIMIT), 0, 1)
        worst_ref[...] = jnp.maximum(jnp.where(slate == 0, late, worst_ref[...]), bad)

    flag_ref[...] = jnp.broadcast_to(jnp.max(worst_ref[...], axis=1, keepdims=True), flag_ref.shape)
    for chunk in range(chunks):
        sent = send_refs[chunk].at[others]
        pltpu.make_async_copy(sent, sent, send_sems.at[chunk]).wait()
        keep(chunk).wait()


def rank(owner, row_index, gains, table, weights, capacity, shards):
    slates, length = owner.shape
    rows, width = table.shape
    model = gains[0].shape[1]
    ends = chunk_ends(capacity)
    depths = [end - start for start, end in zip([0] + ends[:-1], ends)]
    chunks = len(depths)
    vmem, hbm = pl.BlockSpec(memory_space=pltpu.VMEM), pl.BlockSpec(memory_space=pltpu.HBM)
    size = block_size(rows)
    blocks = [(shards, depth, width) for depth in depths]
    tall = max(rows, shards * capacity + 4 * model)
    return pl.pallas_call(
        functools.partial(rank_kernel, capacity),
        out_shape=[
            jax.ShapeDtypeStruct((slates, 1, length), f32),
            jax.ShapeDtypeStruct((1, 128), i32),
            jax.ShapeDtypeStruct((slates, length), i32),
            *[jax.ShapeDtypeStruct(block, bf16) for block in blocks],
        ],
        in_specs=[vmem, vmem, *[vmem] * 3, hbm, *[hbm] * 5],
        out_specs=[vmem, vmem, vmem, *[hbm] * chunks],
        scratch_shapes=[
            pltpu.VMEM((tall, width), f32),
            pltpu.VMEM((BUFFERS, size, width), bf16),
            pltpu.VMEM((shards, 1, capacity), i32),
            pltpu.VMEM((shards, 1, capacity), i32),
            pltpu.SMEM((shards, 1, capacity), i32),
            pltpu.SMEM((slates, length), i32),
            pltpu.VMEM((max(depths), width), f32),
            pltpu.VMEM((length, width), f32),
            pltpu.VMEM((1, length), i32),
            *[pltpu.VMEM(block, bf16) for block in blocks],
            *[pltpu.VMEM(block, bf16) for block in blocks],
            *[pltpu.VMEM(w.shape, bf16) for w in weights],
            *[pltpu.VMEM(w.shape[::-1], bf16) for w in weights],
            *score_scratch(model, length),
            pltpu.SemaphoreType.DMA((BUFFERS,)),
            pltpu.SemaphoreType.DMA((5,)),
            pltpu.SemaphoreType.DMA,
            pltpu.SemaphoreType.DMA,
            pltpu.SemaphoreType.DMA((2,)),
            pltpu.SemaphoreType.DMA((chunks,)),
            pltpu.SemaphoreType.DMA((chunks,)),
            pltpu.SemaphoreType.DMA((chunks,)),
        ],
        compiler_params=pltpu.CompilerParams(
            collective_id=0, has_side_effects=True, vmem_limit_bytes=67043328
        ),
        name="rank",
    )(owner, row_index, *gains, table, *weights)


def finish_kernel(flag_ref, ranked_ref, place_hbm, norm_hbm, final_hbm, score_hbm, *refs):
    raw_hbm, refs = refs[:5], refs[5:]
    chunks = len(refs) - 24
    kept_refs, out_ref, refs = refs[:chunks], refs[chunks], refs[chunks + 1 :]
    rows_ref, landed_ref, emb_ref, place_ref = refs[:4]
    gain_refs, raw, turned, scratch, sem = refs[4:7], refs[7:12], refs[12:17], refs[17:22], refs[22]
    slates, length = out_ref.shape
    model = norm_hbm.shape[1]
    redo = flag_ref[0, 0] > 0

    def fetch(source, target):
        copy = pltpu.make_async_copy(source, target, sem)
        copy.start()
        copy.wait()

    @pl.when(jnp.logical_not(redo))
    def _():
        for slate in range(slates):
            out_ref[slate : slate + 1, :] = ranked_ref[slate]

    @pl.when(redo)
    def _():
        fetch(place_hbm, place_ref)
        for source, target in zip((norm_hbm, final_hbm, score_hbm, *raw_hbm), (*gain_refs, *raw)):
            fetch(source, target)
        turn_weights(raw, turned)
        base = 0
        for kept in kept_refs:
            shards, depth, width = kept.shape
            fetch(kept, landed_ref.at[:, pl.ds(0, depth), :])

            @pl.loop(0, shards)
            def _(peer):
                start = pl.multiple_of(base + peer * depth, 16)
                rows_ref[pl.ds(start, depth), :] = landed_ref[peer, pl.ds(0, depth), :].astype(f32)

            base += shards * depth
        spread_gains(gain_refs, rows_ref, base)
        gain_of = lambda row: widen(rows_ref, base, row, model, length)

        @pl.loop(0, slates)
        def _(slate):
            @pl.loop(0, length // PICK)
            def _(block):
                for row in range(PICK):
                    index = block * PICK + row
                    emb_ref[pl.ds(index, 1), :] = rows_ref[pl.ds(place_ref[slate, index], 1), :]

            result, low, high = score_slate(emb_ref[...].astype(bf16), turned, gain_of, scratch, True)
            out_ref[pl.ds(slate, 1), :] = result


def finish(flag, place, ranked, gains, weights, kept):
    slates, unused, length = ranked.shape
    model = gains[0].shape[1]
    shards, unused, width = kept[0].shape
    deepest = max(block.shape[1] for block in kept)
    capacity = sum(block.shape[1] for block in kept)
    vmem, hbm, smem = [pl.BlockSpec(memory_space=m) for m in (pltpu.VMEM, pltpu.HBM, pltpu.SMEM)]
    return pl.pallas_call(
        finish_kernel,
        out_shape=jax.ShapeDtypeStruct((slates, length), f32),
        in_specs=[smem, vmem, *[hbm] * (9 + len(kept))],
        out_specs=vmem,
        scratch_shapes=[
            pltpu.VMEM((shards * capacity + 4 * model, width), f32),
            pltpu.VMEM((shards, deepest, width), bf16),
            pltpu.VMEM((length, width), f32),
            pltpu.SMEM((slates, length), i32),
            *[pltpu.VMEM(gain.shape, gain.dtype) for gain in gains],
            *[pltpu.VMEM(w.shape, bf16) for w in weights],
            *[pltpu.VMEM(w.shape[::-1], bf16) for w in weights],
            *score_scratch(model, length),
            pltpu.SemaphoreType.DMA,
        ],
        compiler_params=pltpu.CompilerParams(vmem_limit_bytes=60 * 1024 * 1024),
        name="finish",
    )(flag, ranked, place, *gains, *weights, *kept)


def per_device(
    candidate_owner,
    candidate_row,
    item_table,
    w_in,
    w_qkv,
    w_out,
    w_up,
    w_down,
    norm_gains,
    final_gain,
    w_score,
):
    slates, length, unused = candidate_owner.shape
    shards = lax.axis_size(("gx", "gy"))
    capacity = max(16, 2 * slates * length // shards)
    owner = candidate_owner.reshape(slates, length)
    gains = (norm_gains[0], final_gain[None, :], w_score[None, :])
    weights = (w_in, w_qkv[0], w_out[0], w_up[0], w_down[0])
    ranked, flag, place, *kept = rank(owner, candidate_row, gains, item_table, weights, capacity, shards)
    return finish(flag, place, ranked, gains, weights, kept)


def solution(mesh):
    return jax.shard_map(
        per_device,
        mesh=mesh,
        in_specs=(
            P(("gx", "gy"), None, None),
            P(("gx", "gy"), None),
            P(("gx", "gy"), None),
            P(),
            P(),
            P(),
            P(),
            P(),
            P(),
            P(),
            P(),
        ),
        out_specs=P(("gx", "gy"), None),
        check_vma=False,
    )
```

```python
import functools
import math
import jax
import jax.numpy as jnp
from jax import lax
from jax.experimental import pallas as pl
from jax.experimental.pallas import tpu as pltpu
from jax.sharding import PartitionSpec as P

HEADS = 8
PICK = 64
AHEAD = 2
STRIP = 256
PARTS = 4
BUFFERS = 3
EARLY = 5
LOG2E = 1.4426950408889634
LIMIT = 2.0**60
f32, bf16, i32 = jnp.float32, jnp.bfloat16, jnp.int32
MESH = pl.DeviceIdType.MESH


def chunk_ends(capacity):
    return sorted({-(-capacity * part // 128) * 16 for part in (2, 4, 5, 6, 7, 8)})


def ready_chunks(capacity, slates):
    ends, ready = chunk_ends(capacity), []
    for slate in range(slates):
        part = (slate + 1) / slates
        need = min(capacity, capacity * part + 4 * math.sqrt(capacity * part * (1 - part) * (1 - 1 / 16)))
        ready.append(next(chunk for chunk, end in enumerate(ends) if end >= need))
    return ready


def block_size(rows):
    return next(size for size in range(4608, 0, -16) if rows % size == 0)


def norm_parts(ref, cols):
    scale = 1.0 / ref.shape[0]
    mean = jnp.sum(ref[:, cols], axis=0, keepdims=True) * scale
    centred = ref[:, cols] - mean
    variance = jnp.sum(centred * centred, axis=0, keepdims=True) * scale
    return mean, lax.rsqrt(variance + 1e-05)


def norm_into(ref, out_ref, gain_of, row):
    length = ref.shape[1]
    for start in range(0, length, STRIP):
        cols = slice(start, min(start + STRIP, length))
        mean, scale = norm_parts(ref, cols)
        out_ref[:, cols] = ((ref[:, cols] - mean) * scale * gain_of(row, cols.stop - start)).astype(bf16)


def score_slate(emb, weights, gain_of, scratch, exact):
    w_in, w_qkv, w_out, w_up, w_down = weights
    resid_ref, query_ref, keys_ref, value_ref, mixed_ref, normed_ref, inner_ref = scratch
    model, length = w_in.shape[0], emb.shape[0]
    head_dim = model // HEADS
    pack = 128 // head_dim
    resid_ref[...] = lax.dot_general(w_in[...], emb, (((1,), (1,)), ((), ())), preferred_element_type=f32)
    norm_into(resid_ref, normed_ref, gain_of, 0)
    keys = jnp.dot(w_qkv[model : 2 * model], normed_ref[...], preferred_element_type=f32)
    keys_ref[...] = keys.astype(bf16).T
    query = jnp.dot(w_qkv[:model], normed_ref[...], preferred_element_type=f32)
    query_ref[...] = (query * (LOG2E * head_dim ** (-0.5))).astype(bf16)
    value_ref[...] = jnp.dot(w_qkv[2 * model :], normed_ref[...], preferred_element_type=f32).astype(bf16)
    zeros = jnp.zeros((head_dim, length), bf16)
    ones = jnp.ones((16, length), bf16)

    def scores_of(head):
        group, part = head // pack, head % pack
        query = query_ref[head * head_dim : (head + 1) * head_dim, :]
        query = jnp.concatenate([query if p == part else zeros for p in range(pack)], axis=0)
        return jnp.dot(keys_ref[:, group * 128 : (group + 1) * 128], query, preferred_element_type=f32)

    low = high = None
    ahead = scores_of(0)
    for head in range(HEADS):
        rows = slice(head * head_dim, (head + 1) * head_dim)
        scores = ahead
        if head + 1 < HEADS:
            ahead = scores_of(head + 1)
        if exact:
            scores = scores - jnp.max(scores, axis=0, keepdims=True)
        probs = jnp.exp2(scores).astype(bf16)
        stacked = jnp.concatenate([value_ref[rows, :], ones], axis=0)
        both = jnp.dot(stacked, probs, preferred_element_type=f32)
        total = both[head_dim : head_dim + 1]
        low = total if low is None else jnp.minimum(low, total)
        high = total if high is None else jnp.maximum(high, total)
        mixed_ref[rows, :] = (both[:head_dim] * (1.0 / total)).astype(bf16)
    resid_ref[...] = resid_ref[...] + jnp.dot(w_out[...], mixed_ref[...], preferred_element_type=f32)
    norm_into(resid_ref, normed_ref, gain_of, 1)
    part = w_up.shape[0] // PARTS
    for start in range(0, part * PARTS, part):
        inner = jnp.dot(w_up[start : start + part], normed_ref[...], preferred_element_type=f32)
        half = 0.5 * inner
        inner = half + half * jnp.tanh(inner * (0.7978845608028654 + 0.035677408136300125 * (inner * inner)))
        inner_ref[start : start + part] = inner.astype(bf16)
    resid_ref[...] = resid_ref[...] + jnp.dot(w_down[...], inner_ref[...], preferred_element_type=f32)
    pieces = []
    for start in range(0, length, 128):
        cols = slice(start, start + 128)
        mean, scale = norm_parts(resid_ref, cols)
        terms = (resid_ref[:, cols] - mean) * (gain_of(2, 128) * gain_of(3, 128))
        pieces.append(jnp.sum(terms, axis=0, keepdims=True) * scale)
    logits = jnp.concatenate(pieces, axis=1)
    shifted = logits - jnp.max(logits, axis=-1, keepdims=True)
    result = shifted - jnp.log(jnp.sum(jnp.exp(shifted), axis=-1, keepdims=True))
    return result, low, high


def score_scratch(model, length, inner):
    return [
        pltpu.VMEM((model, length), f32),
        pltpu.VMEM((model, length), bf16),
        pltpu.VMEM((length, model), bf16),
        pltpu.VMEM((model, length), bf16),
        pltpu.VMEM((model, length), bf16),
        pltpu.VMEM((model, length), bf16),
        pltpu.VMEM((inner, length), bf16),
    ]


def turn_weights(raw, turned):
    for source, target in zip(raw, turned):
        rows, cols = source.shape
        for row in range(0, rows, 512):
            for col in range(0, cols, 512):
                r, c = slice(row, min(rows, row + 512)), slice(col, min(cols, col + 512))
                target[c, r] = source[r, c].T


def spread_gains(gain_refs, target, base):
    norm_ref, final_ref, score_ref = gain_refs
    model = norm_ref.shape[1]
    gains = [norm_ref[...], final_ref[...], score_ref[...].astype(f32)[None, :], jnp.zeros((4, model), f32)]
    columns = jnp.concatenate(gains, axis=0).T
    for row in range(4):
        target[base + row * model : base + (row + 1) * model, :] = jnp.broadcast_to(
            columns[:, row : row + 1], (model, 128)
        )


def widen(gains_ref, base, row, model, length):
    gain = gains_ref[base + row * model : base + (row + 1) * model, :]
    return jnp.concatenate([gain] * (length // 128), axis=1)


def route(owner_ref, row_ref, asks_ref, place_ref, capacity, shards, rows, bounds):
    slates, unused, length = owner_ref.shape
    ends = chunk_ends(capacity)
    shard = lax.broadcasted_iota(i32, (shards, length), 0)
    slots = lax.broadcasted_iota(i32, (capacity, length), 0)
    upper = lax.broadcasted_iota(i32, (length, length), 0) <= lax.broadcasted_iota(i32, (length, length), 1)
    upper = upper.astype(f32).astype(bf16)
    hits = [(owner_ref[b] == shard).astype(f32) for b in range(slates)]
    within = jnp.dot(jnp.concatenate(hits, axis=0).astype(bf16), upper, preferred_element_type=f32)
    before = jnp.zeros((shards, 1), f32)
    found, late = None, None
    for b in range(slates):
        counts = within[b * shards : (b + 1) * shards]
        slot = jnp.sum(hits[b] * (counts + before), axis=0, keepdims=True).astype(i32) - 1
        before = before + counts[:, length - 1 : length]
        owner, index = owner_ref[b], row_ref[b : b + 1, :]
        place = owner * ends[0] + slot
        for start, end in zip(ends[:-1], ends[1:]):
            here = shards * start + owner * (end - start) + (slot - start)
            place = jnp.where(slot >= start, here, place)
        place_ref[b] = jnp.clip(place, 0, shards * capacity - 1)
        over = (slot >= bounds[b]).astype(i32)
        late = over if late is None else jnp.maximum(late, over)
        at_slot = (slot == slots).astype(f32).astype(bf16)
        digits = (index >> 16, (index >> 8) & 255, index & 255)
        placed = jnp.concatenate([hits[b] * digit.astype(f32) for digit in digits], axis=0).astype(bf16)
        part = lax.dot_general(placed, at_slot, (((1,), (1,)), ((), ())), preferred_element_type=f32)
        found = part if found is None else found + part
    found = found.astype(i32)
    asks = (found[:shards] << 16) + (found[shards : 2 * shards] << 8) + found[2 * shards :]
    asks = jnp.clip(asks, 0, rows - 1)
    for peer in range(shards):
        asks_ref[peer] = asks[peer : peer + 1, :]
    return late


def rank_kernel(capacity, owner_ref, row_ref, norm_ref, final_ref, score_ref, table_ref, *refs):
    chunks = len(chunk_ends(capacity))
    raw_hbm, refs = refs[:5], refs[5:]
    out_ref, flag_ref, place_ref = refs[:3]
    kept_refs, refs = refs[3 : 3 + chunks], refs[3 + chunks :]
    rows_ref, stream_ref, asks_ref, wanted_ref, wanted_smem, place_smem, stage_ref, emb_ref, worst_ref = refs[:9]
    send_refs, refs = refs[9 : 9 + chunks], refs[9 + chunks :]
    recv_refs, refs = refs[:chunks], refs[chunks:]
    raw, turned, refs = refs[:5], refs[5:10], refs[10:]
    scratch, refs = refs[:7], refs[7:]
    (
        stream_sems, raw_sems, ask_send_sem, ask_recv_sem, smem_sems,
        send_sems, recv_sems, keep_sems,
    ) = refs
    inner = lax.axis_size("gy")
    count = lax.axis_size("gx") * inner
    here = lax.axis_index("gx") * inner + lax.axis_index("gy")
    slates, unused, length = owner_ref.shape
    model = norm_ref.shape[1]
    ends = chunk_ends(capacity)
    starts = [0] + ends[:-1]
    ready = ready_chunks(capacity, slates)
    barrier = pltpu.get_barrier_semaphore()

    def peer_of(step):
        peer = lax.rem(here + step, count)
        return peer, (peer // inner, lax.rem(peer, inner))

    @pl.loop(1, count)
    def _(step):
        pl.semaphore_signal(barrier, inc=1, device_id=peer_of(step)[1], device_id_type=MESH)

    size = stream_ref.shape[1]
    blocks = table_ref.shape[0] // size

    def stream(block):
        slot = lax.rem(block, BUFFERS)
        return pltpu.make_async_copy(
            table_ref.at[pl.ds(pl.multiple_of(block * size, size), size)], stream_ref.at[slot], stream_sems.at[slot]
        )

    for block in range(min(BUFFERS, blocks)):
        stream(block).start()
    copies = [pltpu.make_async_copy(s, t, raw_sems.at[n]) for n, (s, t) in enumerate(zip(raw_hbm, raw))]
    for copy in copies:
        copy.start()

    def load(block):
        stream(block).wait()
        start = pl.multiple_of(block * size, size)
        rows_ref[pl.ds(start, size), :] = stream_ref[lax.rem(block, BUFFERS)].astype(f32)

        @pl.when(block + BUFFERS < blocks)
        def _():
            stream(block + BUFFERS).start()

    late = route(
        owner_ref, row_ref, asks_ref, place_ref, capacity, count, table_ref.shape[0], [ends[chunk] for chunk in ready]
    )
    place_copy = pltpu.make_async_copy(place_ref, place_smem, smem_sems.at[0])
    place_copy.start()

    early = min(EARLY, blocks)

    @pl.loop(0, early)
    def _(block):
        load(block)

    def ask(step):
        peer, device = peer_of(step)
        return pltpu.make_async_remote_copy(
            src_ref=asks_ref.at[peer],
            dst_ref=wanted_ref.at[here],
            send_sem=ask_send_sem,
            recv_sem=ask_recv_sem,
            device_id=device,
            device_id_type=MESH,
        )

    pl.semaphore_wait(barrier, count - 1)

    @pl.loop(1, count)
    def _(step):
        ask(step).start()

    wanted_ref[here] = asks_ref[here]

    @pl.loop(early, blocks)
    def _(block):
        load(block)

    others = pl.ds(0, count - 1)
    pltpu.make_async_copy(asks_ref.at[others], asks_ref.at[others], ask_send_sem).wait()
    pltpu.make_async_copy(wanted_ref.at[others], wanted_ref.at[others], ask_recv_sem).wait()
    wanted_copy = pltpu.make_async_copy(wanted_ref, wanted_smem, smem_sems.at[1])
    wanted_copy.start()
    wanted_copy.wait()

    def give(chunk, step):
        peer, device = peer_of(step)
        return pltpu.make_async_remote_copy(
            src_ref=send_refs[chunk].at[peer],
            dst_ref=recv_refs[chunk].at[here],
            send_sem=send_sems.at[chunk],
            recv_sem=recv_sems.at[chunk],
            device_id=device,
            device_id_type=MESH,
        )

    def pick(chunk, step):
        peer = peer_of(step)[0]
        depth = ends[chunk] - starts[chunk]
        for row in range(depth):
            index = wanted_smem[peer, 0, starts[chunk] + row]
            stage_ref[row : row + 1, :] = rows_ref[pl.ds(index, 1), :]
        send_refs[chunk][peer] = stage_ref[:depth, :].astype(bf16)

    first = [next(s for s in range(slates) if ready[s] >= chunk) for chunk in range(chunks)]
    later = [chunk for chunk in range(AHEAD, chunks) if first[chunk] > chunk - AHEAD]
    for chunk in range(chunks):

        @pl.loop(1, count)
        def _(step):
            pick(chunk, step)
            if chunk not in later:
                give(chunk, step).start()

        pick(chunk, 0)

    place_copy.wait()
    for copy in copies:
        copy.wait()
    turn_weights(raw, turned)
    gains_base = count * capacity
    spread_gains((norm_ref, final_ref, score_ref), rows_ref, gains_base)

    def keep(chunk):
        return pltpu.make_async_copy(recv_refs[chunk], kept_refs[chunk], keep_sems.at[chunk])

    def take(chunk):
        depth, base = ends[chunk] - starts[chunk], count * starts[chunk]
        landed = recv_refs[chunk]
        pltpu.make_async_copy(landed.at[others], landed.at[others], recv_sems.at[chunk]).wait()
        landed[here] = send_refs[chunk][here]
        keep(chunk).start()

        @pl.loop(0, count)
        def _(peer):
            start = pl.multiple_of(base + peer * depth, 16)
            rows_ref[pl.ds(start, depth), :] = landed[peer].astype(f32)

    @pl.loop(0, slates)
    def _(slate):
        for chunk in range(chunks):

            @pl.when(slate == first[chunk])
            def _():
                take(chunk)

        for chunk in later:

            @pl.when(slate == chunk - AHEAD)
            def _():
                @pl.loop(1, count)
                def _(step):
                    give(chunk, step).start()

        @pl.loop(0, length // PICK)
        def _(block):
            for row in range(PICK):
                index = block * PICK + row
                emb_ref[pl.ds(index, 1), :] = rows_ref[pl.ds(place_smem[slate, 0, index], 1), :]

        gain_of = lambda row, cols: widen(rows_ref, gains_base, row, model, cols)
        result, low, high = score_slate(emb_ref[...].astype(bf16), turned, gain_of, scratch, False)
        out_ref[slate] = result
        bad = jnp.where((low > 1.0 / LIMIT) & (high < LIMIT), 0, 1)
        worst_ref[...] = jnp.maximum(jnp.where(slate == 0, late, worst_ref[...]), bad)

    flag_ref[...] = jnp.broadcast_to(jnp.max(worst_ref[...], axis=1, keepdims=True), flag_ref.shape)
    for chunk in range(chunks):
        sent = send_refs[chunk].at[others]
        pltpu.make_async_copy(sent, sent, send_sems.at[chunk]).wait()
        keep(chunk).wait()


def rank(owner, row_index, gains, table, weights, capacity, shards):
    slates, unused, length = owner.shape
    rows, width = table.shape
    model = gains[0].shape[1]
    ends = chunk_ends(capacity)
    depths = [end - start for start, end in zip([0] + ends[:-1], ends)]
    chunks = len(depths)
    vmem, hbm = pl.BlockSpec(memory_space=pltpu.VMEM), pl.BlockSpec(memory_space=pltpu.HBM)
    size = block_size(rows)
    blocks = [(shards, depth, width) for depth in depths]
    tall = max(rows, shards * capacity + 4 * model)
    return pl.pallas_call(
        functools.partial(rank_kernel, capacity),
        out_shape=[
            jax.ShapeDtypeStruct((slates, 1, length), f32),
            jax.ShapeDtypeStruct((1, 128), i32),
            jax.ShapeDtypeStruct((slates, 1, length), i32),
            *[jax.ShapeDtypeStruct(block, bf16) for block in blocks],
        ],
        in_specs=[vmem, vmem, *[vmem] * 3, hbm, *[hbm] * 5],
        out_specs=[vmem, vmem, vmem, *[hbm] * chunks],
        scratch_shapes=[
            pltpu.VMEM((tall, width), f32),
            pltpu.VMEM((BUFFERS, size, width), bf16),
            pltpu.VMEM((shards, 1, capacity), i32),
            pltpu.VMEM((shards, 1, capacity), i32),
            pltpu.SMEM((shards, 1, capacity), i32),
            pltpu.SMEM((slates, 1, length), i32),
            pltpu.VMEM((max(depths), width), f32),
            pltpu.VMEM((length, width), f32),
            pltpu.VMEM((1, length), i32),
            *[pltpu.VMEM(block, bf16) for block in blocks],
            *[pltpu.VMEM(block, bf16) for block in blocks],
            *[pltpu.VMEM(w.shape, bf16) for w in weights],
            *[pltpu.VMEM(w.shape[::-1], bf16) for w in weights],
            *score_scratch(model, length, weights[3].shape[1]),
            pltpu.SemaphoreType.DMA((BUFFERS,)),
            pltpu.SemaphoreType.DMA((5,)),
            pltpu.SemaphoreType.DMA,
            pltpu.SemaphoreType.DMA,
            pltpu.SemaphoreType.DMA((2,)),
            pltpu.SemaphoreType.DMA((chunks,)),
            pltpu.SemaphoreType.DMA((chunks,)),
            pltpu.SemaphoreType.DMA((chunks,)),
        ],
        compiler_params=pltpu.CompilerParams(
            collective_id=0, has_side_effects=True, vmem_limit_bytes=67043328
        ),
        name="rank",
    )(owner, row_index, *gains, table, *weights)


def finish_kernel(flag_ref, ranked_ref, place_hbm, norm_hbm, final_hbm, score_hbm, *refs):
    raw_hbm, refs = refs[:5], refs[5:]
    chunks = len(refs) - 26
    kept_refs, out_ref, refs = refs[:chunks], refs[chunks], refs[chunks + 1 :]
    rows_ref, landed_ref, emb_ref, place_ref = refs[:4]
    gain_refs, raw, turned, scratch, sem = refs[4:7], refs[7:12], refs[12:17], refs[17:24], refs[24]
    slates, length = out_ref.shape
    model = norm_hbm.shape[1]
    redo = flag_ref[0, 0] > 0

    def fetch(source, target):
        copy = pltpu.make_async_copy(source, target, sem)
        copy.start()
        copy.wait()

    @pl.when(jnp.logical_not(redo))
    def _():
        for slate in range(slates):
            out_ref[slate : slate + 1, :] = ranked_ref[slate]

    @pl.when(redo)
    def _():
        fetch(place_hbm, place_ref)
        for source, target in zip((norm_hbm, final_hbm, score_hbm, *raw_hbm), (*gain_refs, *raw)):
            fetch(source, target)
        turn_weights(raw, turned)
        base = 0
        for kept in kept_refs:
            shards, depth, width = kept.shape
            fetch(kept, landed_ref.at[:, pl.ds(0, depth), :])

            @pl.loop(0, shards)
            def _(peer):
                start = pl.multiple_of(base + peer * depth, 16)
                rows_ref[pl.ds(start, depth), :] = landed_ref[peer, pl.ds(0, depth), :].astype(f32)

            base += shards * depth
        spread_gains(gain_refs, rows_ref, base)
        gain_of = lambda row, cols: widen(rows_ref, base, row, model, cols)

        @pl.loop(0, slates)
        def _(slate):
            @pl.loop(0, length // PICK)
            def _(block):
                for row in range(PICK):
                    index = block * PICK + row
                    emb_ref[pl.ds(index, 1), :] = rows_ref[pl.ds(place_ref[slate, 0, index], 1), :]

            result, low, high = score_slate(emb_ref[...].astype(bf16), turned, gain_of, scratch, True)
            out_ref[pl.ds(slate, 1), :] = result


def finish(flag, place, ranked, gains, weights, kept):
    slates, unused, length = ranked.shape
    model = gains[0].shape[1]
    shards, unused, width = kept[0].shape
    deepest = max(block.shape[1] for block in kept)
    capacity = sum(block.shape[1] for block in kept)
    vmem, hbm, smem = [pl.BlockSpec(memory_space=m) for m in (pltpu.VMEM, pltpu.HBM, pltpu.SMEM)]
    return pl.pallas_call(
        finish_kernel,
        out_shape=jax.ShapeDtypeStruct((slates, length), f32),
        in_specs=[smem, vmem, *[hbm] * (9 + len(kept))],
        out_specs=vmem,
        scratch_shapes=[
            pltpu.VMEM((shards * capacity + 4 * model, width), f32),
            pltpu.VMEM((shards, deepest, width), bf16),
            pltpu.VMEM((length, width), f32),
            pltpu.SMEM((slates, 1, length), i32),
            *[pltpu.VMEM(gain.shape, gain.dtype) for gain in gains],
            *[pltpu.VMEM(w.shape, bf16) for w in weights],
            *[pltpu.VMEM(w.shape[::-1], bf16) for w in weights],
            *score_scratch(model, length, weights[3].shape[1]),
            pltpu.SemaphoreType.DMA,
        ],
        compiler_params=pltpu.CompilerParams(vmem_limit_bytes=60 * 1024 * 1024),
        name="finish",
    )(flag, ranked, place, *gains, *weights, *kept)


def per_device(
    candidate_owner,
    candidate_row,
    item_table,
    w_in,
    w_qkv,
    w_out,
    w_up,
    w_down,
    norm_gains,
    final_gain,
    w_score,
):
    slates, length, unused = candidate_owner.shape
    shards = lax.axis_size(("gx", "gy"))
    capacity = max(16, 2 * slates * length // shards)
    owner = candidate_owner.reshape(slates, 1, length)
    gains = (norm_gains[0], final_gain[None, :], w_score)
    weights = (w_in, w_qkv[0], w_out[0], w_up[0], w_down[0])
    ranked, flag, place, *kept = rank(owner, candidate_row, gains, item_table, weights, capacity, shards)
    return finish(flag, place, ranked, gains, weights, kept)


def solution(mesh):
    return jax.shard_map(
        per_device,
        mesh=mesh,
        in_specs=(
            P(("gx", "gy"), None, None),
            P(("gx", "gy"), None),
            P(("gx", "gy"), None),
            P(),
            P(),
            P(),
            P(),
            P(),
            P(),
            P(),
            P(),
        ),
        out_specs=P(("gx", "gy"), None),
        check_vma=False,
    )
```

```python
import functools
import math
import jax
import jax.numpy as jnp
from jax import lax
from jax.experimental import pallas as pl
from jax.experimental.pallas import tpu as pltpu
from jax.sharding import PartitionSpec as P

HEADS = 8
PICK = 64
AHEAD = 2
STRIP = 256
PARTS = 4
BUFFERS = 3
EARLY = 5
LOG2E = 1.4426950408889634
LIMIT = 2.0**60
f32, bf16, i32 = jnp.float32, jnp.bfloat16, jnp.int32
MESH = pl.DeviceIdType.MESH


def chunk_ends(capacity):
    return sorted({-(-capacity * part // 128) * 16 for part in (2, 3, 4, 5, 6, 7, 8)})


def ready_chunks(capacity, slates):
    ends, ready = chunk_ends(capacity), []
    for slate in range(slates):
        part = (slate + 1) / slates
        need = min(capacity, capacity * part + 4 * math.sqrt(capacity * part * (1 - part) * (1 - 1 / 16)))
        ready.append(next(chunk for chunk, end in enumerate(ends) if end >= need))
    return ready


def block_size(rows):
    return next(size for size in range(4608, 0, -16) if rows % size == 0)


def norm_parts(ref, cols):
    scale = 1.0 / ref.shape[0]
    mean = jnp.sum(ref[:, cols], axis=0, keepdims=True) * scale
    centred = ref[:, cols] - mean
    variance = jnp.sum(centred * centred, axis=0, keepdims=True) * scale
    return mean, lax.rsqrt(variance + 1e-05)


def norm_into(ref, out_ref, gain_of, row):
    length = ref.shape[1]
    for start in range(0, length, STRIP):
        cols = slice(start, min(start + STRIP, length))
        mean, scale = norm_parts(ref, cols)
        out_ref[:, cols] = ((ref[:, cols] - mean) * scale * gain_of(row, cols.stop - start)).astype(bf16)


def score_slate(emb, weights, gain_of, scratch, exact):
    w_in, w_qkv, w_out, w_up, w_down = weights
    resid_ref, query_ref, keys_ref, value_ref, mixed_ref, normed_ref, inner_ref = scratch
    model, length = w_in.shape[0], emb.shape[0]
    head_dim = model // HEADS
    pack = 128 // head_dim
    resid_ref[...] = lax.dot_general(w_in[...], emb, (((1,), (1,)), ((), ())), preferred_element_type=f32)
    norm_into(resid_ref, normed_ref, gain_of, 0)
    keys = jnp.dot(w_qkv[model : 2 * model], normed_ref[...], preferred_element_type=f32)
    keys_ref[...] = keys.astype(bf16).T
    query = jnp.dot(w_qkv[:model], normed_ref[...], preferred_element_type=f32)
    query_ref[...] = (query * (LOG2E * head_dim ** (-0.5))).astype(bf16)
    value_ref[...] = jnp.dot(w_qkv[2 * model :], normed_ref[...], preferred_element_type=f32).astype(bf16)
    zeros = jnp.zeros((head_dim, length), bf16)
    ones = jnp.ones((16, length), bf16)

    def scores_of(head):
        group, part = head // pack, head % pack
        query = query_ref[head * head_dim : (head + 1) * head_dim, :]
        query = jnp.concatenate([query if p == part else zeros for p in range(pack)], axis=0)
        return jnp.dot(keys_ref[:, group * 128 : (group + 1) * 128], query, preferred_element_type=f32)

    low = high = None
    ahead = scores_of(0)
    for head in range(HEADS):
        rows = slice(head * head_dim, (head + 1) * head_dim)
        scores = ahead
        if head + 1 < HEADS:
            ahead = scores_of(head + 1)
        if exact:
            scores = scores - jnp.max(scores, axis=0, keepdims=True)
        probs = jnp.exp2(scores).astype(bf16)
        stacked = jnp.concatenate([value_ref[rows, :], ones], axis=0)
        both = jnp.dot(stacked, probs, preferred_element_type=f32)
        total = both[head_dim : head_dim + 1]
        low = total if low is None else jnp.minimum(low, total)
        high = total if high is None else jnp.maximum(high, total)
        mixed_ref[rows, :] = (both[:head_dim] * (1.0 / total)).astype(bf16)
    resid_ref[...] = resid_ref[...] + jnp.dot(w_out[...], mixed_ref[...], preferred_element_type=f32)
    norm_into(resid_ref, normed_ref, gain_of, 1)
    part = w_up.shape[0] // PARTS
    for start in range(0, part * PARTS, part):
        inner = jnp.dot(w_up[start : start + part], normed_ref[...], preferred_element_type=f32)
        half = 0.5 * inner
        inner = half + half * jnp.tanh(inner * (0.7978845608028654 + 0.035677408136300125 * (inner * inner)))
        inner_ref[start : start + part] = inner.astype(bf16)
    resid_ref[...] = resid_ref[...] + jnp.dot(w_down[...], inner_ref[...], preferred_element_type=f32)
    pieces = []
    for start in range(0, length, 128):
        cols = slice(start, start + 128)
        mean, scale = norm_parts(resid_ref, cols)
        terms = (resid_ref[:, cols] - mean) * (gain_of(2, 128) * gain_of(3, 128))
        pieces.append(jnp.sum(terms, axis=0, keepdims=True) * scale)
    logits = jnp.concatenate(pieces, axis=1)
    shifted = logits - jnp.max(logits, axis=-1, keepdims=True)
    result = shifted - jnp.log(jnp.sum(jnp.exp(shifted), axis=-1, keepdims=True))
    return result, low, high


def score_scratch(model, length, inner):
    return [
        pltpu.VMEM((model, length), f32),
        pltpu.VMEM((model, length), bf16),
        pltpu.VMEM((length, model), bf16),
        pltpu.VMEM((model, length), bf16),
        pltpu.VMEM((model, length), bf16),
        pltpu.VMEM((model, length), bf16),
        pltpu.VMEM((inner, length), bf16),
    ]


def turn_weights(raw, turned):
    for source, target in zip(raw, turned):
        rows, cols = source.shape
        for row in range(0, rows, 512):
            for col in range(0, cols, 512):
                r, c = slice(row, min(rows, row + 512)), slice(col, min(cols, col + 512))
                target[c, r] = source[r, c].T


def spread_gains(gain_refs, target, base):
    norm_ref, final_ref, score_ref = gain_refs
    model = norm_ref.shape[1]
    gains = [norm_ref[...], final_ref[...], score_ref[...].astype(f32)[None, :], jnp.zeros((4, model), f32)]
    columns = jnp.concatenate(gains, axis=0).T
    for row in range(4):
        target[base + row * model : base + (row + 1) * model, :] = jnp.broadcast_to(
            columns[:, row : row + 1], (model, 128)
        )


def widen(gains_ref, base, row, model, length):
    gain = gains_ref[base + row * model : base + (row + 1) * model, :]
    return jnp.concatenate([gain] * (length // 128), axis=1)


def route(owner_ref, row_ref, asks_ref, place_ref, capacity, shards, rows, bounds):
    slates, unused, length = owner_ref.shape
    ends = chunk_ends(capacity)
    shard = lax.broadcasted_iota(i32, (shards, length), 0)
    slots = lax.broadcasted_iota(i32, (capacity, length), 0)
    upper = lax.broadcasted_iota(i32, (length, length), 0) <= lax.broadcasted_iota(i32, (length, length), 1)
    upper = upper.astype(f32).astype(bf16)
    hits = [(owner_ref[b] == shard).astype(f32) for b in range(slates)]
    within = jnp.dot(jnp.concatenate(hits, axis=0).astype(bf16), upper, preferred_element_type=f32)
    before = jnp.zeros((shards, 1), f32)
    found, late = None, None
    for b in range(slates):
        counts = within[b * shards : (b + 1) * shards]
        slot = jnp.sum(hits[b] * (counts + before), axis=0, keepdims=True).astype(i32) - 1
        before = before + counts[:, length - 1 : length]
        owner, index = owner_ref[b], row_ref[b : b + 1, :]
        place = owner * ends[0] + slot
        for start, end in zip(ends[:-1], ends[1:]):
            here = shards * start + owner * (end - start) + (slot - start)
            place = jnp.where(slot >= start, here, place)
        place_ref[b] = jnp.clip(place, 0, shards * capacity - 1)
        over = (slot >= bounds[b]).astype(i32)
        late = over if late is None else jnp.maximum(late, over)
        at_slot = (slot == slots).astype(f32).astype(bf16)
        digits = (index >> 16, (index >> 8) & 255, index & 255)
        placed = jnp.concatenate([hits[b] * digit.astype(f32) for digit in digits], axis=0).astype(bf16)
        part = lax.dot_general(placed, at_slot, (((1,), (1,)), ((), ())), preferred_element_type=f32)
        found = part if found is None else found + part
    found = found.astype(i32)
    asks = (found[:shards] << 16) + (found[shards : 2 * shards] << 8) + found[2 * shards :]
    asks = jnp.clip(asks, 0, rows - 1)
    for peer in range(shards):
        asks_ref[peer] = asks[peer : peer + 1, :]
    return late


def rank_kernel(capacity, owner_ref, row_ref, norm_ref, final_ref, score_ref, table_ref, *refs):
    chunks = len(chunk_ends(capacity))
    raw_hbm, refs = refs[:5], refs[5:]
    out_ref, flag_ref, place_ref = refs[:3]
    kept_refs, refs = refs[3 : 3 + chunks], refs[3 + chunks :]
    rows_ref, stream_ref, asks_ref, wanted_ref, wanted_smem, place_smem, stage_ref, emb_ref, worst_ref = refs[:9]
    send_refs, refs = refs[9 : 9 + chunks], refs[9 + chunks :]
    recv_refs, refs = refs[:chunks], refs[chunks:]
    raw, turned, refs = refs[:5], refs[5:10], refs[10:]
    scratch, refs = refs[:7], refs[7:]
    (
        stream_sems, raw_sems, ask_send_sem, ask_recv_sem, smem_sems,
        send_sems, recv_sems, keep_sems,
    ) = refs
    inner = lax.axis_size("gy")
    count = lax.axis_size("gx") * inner
    here = lax.axis_index("gx") * inner + lax.axis_index("gy")
    slates, unused, length = owner_ref.shape
    model = norm_ref.shape[1]
    ends = chunk_ends(capacity)
    starts = [0] + ends[:-1]
    ready = ready_chunks(capacity, slates)
    barrier = pltpu.get_barrier_semaphore()

    def peer_of(step):
        peer = lax.rem(here + step, count)
        return peer, (peer // inner, lax.rem(peer, inner))

    @pl.loop(1, count)
    def _(step):
        pl.semaphore_signal(barrier, inc=1, device_id=peer_of(step)[1], device_id_type=MESH)

    size = stream_ref.shape[1]
    blocks = table_ref.shape[0] // size

    def stream(block):
        slot = lax.rem(block, BUFFERS)
        return pltpu.make_async_copy(
            table_ref.at[pl.ds(pl.multiple_of(block * size, size), size)], stream_ref.at[slot], stream_sems.at[slot]
        )

    for block in range(min(BUFFERS, blocks)):
        stream(block).start()
    copies = [pltpu.make_async_copy(s, t, raw_sems.at[n]) for n, (s, t) in enumerate(zip(raw_hbm, raw))]
    for copy in copies:
        copy.start()

    def load(block):
        stream(block).wait()
        start = pl.multiple_of(block * size, size)
        rows_ref[pl.ds(start, size), :] = stream_ref[lax.rem(block, BUFFERS)].astype(f32)

        @pl.when(block + BUFFERS < blocks)
        def _():
            stream(block + BUFFERS).start()

    late = route(
        owner_ref, row_ref, asks_ref, place_ref, capacity, count, table_ref.shape[0], [ends[chunk] for chunk in ready]
    )
    place_copy = pltpu.make_async_copy(place_ref, place_smem, smem_sems.at[0])
    place_copy.start()

    early = min(EARLY, blocks)

    @pl.loop(0, early)
    def _(block):
        load(block)

    def ask(step):
        peer, device = peer_of(step)
        return pltpu.make_async_remote_copy(
            src_ref=asks_ref.at[peer],
            dst_ref=wanted_ref.at[here],
            send_sem=ask_send_sem,
            recv_sem=ask_recv_sem,
            device_id=device,
            device_id_type=MESH,
        )

    pl.semaphore_wait(barrier, count - 1)

    @pl.loop(1, count)
    def _(step):
        ask(step).start()

    wanted_ref[here] = asks_ref[here]

    @pl.loop(early, blocks)
    def _(block):
        load(block)

    others = pl.ds(0, count - 1)
    pltpu.make_async_copy(asks_ref.at[others], asks_ref.at[others], ask_send_sem).wait()
    pltpu.make_async_copy(wanted_ref.at[others], wanted_ref.at[others], ask_recv_sem).wait()
    wanted_copy = pltpu.make_async_copy(wanted_ref, wanted_smem, smem_sems.at[1])
    wanted_copy.start()
    wanted_copy.wait()

    def give(chunk, step):
        peer, device = peer_of(step)
        return pltpu.make_async_remote_copy(
            src_ref=send_refs[chunk].at[peer],
            dst_ref=recv_refs[chunk].at[here],
            send_sem=send_sems.at[chunk],
            recv_sem=recv_sems.at[chunk],
            device_id=device,
            device_id_type=MESH,
        )

    def pick(chunk, step):
        peer = peer_of(step)[0]
        depth = ends[chunk] - starts[chunk]
        for row in range(depth):
            index = wanted_smem[peer, 0, starts[chunk] + row]
            stage_ref[row : row + 1, :] = rows_ref[pl.ds(index, 1), :]
        send_refs[chunk][peer] = stage_ref[:depth, :].astype(bf16)

    first = [next(s for s in range(slates) if ready[s] >= chunk) for chunk in range(chunks)]
    later = [chunk for chunk in range(AHEAD, chunks) if first[chunk] > chunk - AHEAD]
    for chunk in range(chunks):

        @pl.loop(1, count)
        def _(step):
            pick(chunk, step)
            if chunk not in later:
                give(chunk, step).start()

        pick(chunk, 0)

    place_copy.wait()
    for copy in copies:
        copy.wait()
    turn_weights(raw, turned)
    gains_base = count * capacity
    spread_gains((norm_ref, final_ref, score_ref), rows_ref, gains_base)

    def keep(chunk):
        return pltpu.make_async_copy(recv_refs[chunk], kept_refs[chunk], keep_sems.at[chunk])

    def take(chunk):
        depth, base = ends[chunk] - starts[chunk], count * starts[chunk]
        landed = recv_refs[chunk]
        pltpu.make_async_copy(landed.at[others], landed.at[others], recv_sems.at[chunk]).wait()
        landed[here] = send_refs[chunk][here]
        keep(chunk).start()

        @pl.loop(0, count)
        def _(peer):
            start = pl.multiple_of(base + peer * depth, 16)
            rows_ref[pl.ds(start, depth), :] = landed[peer].astype(f32)

    @pl.loop(0, slates)
    def _(slate):
        for chunk in range(chunks):

            @pl.when(slate == first[chunk])
            def _():
                take(chunk)

        for chunk in later:

            @pl.when(slate == chunk - AHEAD)
            def _():
                @pl.loop(1, count)
                def _(step):
                    give(chunk, step).start()

        @pl.loop(0, length // PICK)
        def _(block):
            start = pl.multiple_of(block * PICK, PICK)
            for row in range(PICK):
                index = place_smem[slate, 0, start + row]
                stage_ref[row : row + 1, :] = rows_ref[pl.ds(index, 1), :]
            emb_ref[pl.ds(start, PICK), :] = stage_ref[:PICK, :].astype(bf16)

        gain_of = lambda row, cols: widen(rows_ref, gains_base, row, model, cols)
        result, low, high = score_slate(emb_ref[...], turned, gain_of, scratch, False)
        out_ref[slate] = result
        bad = jnp.where((low > 1.0 / LIMIT) & (high < LIMIT), 0, 1)
        worst_ref[...] = jnp.maximum(jnp.where(slate == 0, late, worst_ref[...]), bad)

    flag_ref[...] = jnp.broadcast_to(jnp.max(worst_ref[...], axis=1, keepdims=True), flag_ref.shape)
    for chunk in range(chunks):
        sent = send_refs[chunk].at[others]
        pltpu.make_async_copy(sent, sent, send_sems.at[chunk]).wait()
        keep(chunk).wait()


def rank(owner, row_index, gains, table, weights, capacity, shards):
    slates, unused, length = owner.shape
    rows, width = table.shape
    model = gains[0].shape[1]
    ends = chunk_ends(capacity)
    depths = [end - start for start, end in zip([0] + ends[:-1], ends)]
    chunks = len(depths)
    vmem, hbm = pl.BlockSpec(memory_space=pltpu.VMEM), pl.BlockSpec(memory_space=pltpu.HBM)
    size = block_size(rows)
    blocks = [(shards, depth, width) for depth in depths]
    tall = max(rows, shards * capacity + 4 * model)
    return pl.pallas_call(
        functools.partial(rank_kernel, capacity),
        out_shape=[
            jax.ShapeDtypeStruct((slates, 1, length), f32),
            jax.ShapeDtypeStruct((1, 128), i32),
            jax.ShapeDtypeStruct((slates, 1, length), i32),
            *[jax.ShapeDtypeStruct(block, bf16) for block in blocks],
        ],
        in_specs=[vmem, vmem, *[vmem] * 3, hbm, *[hbm] * 5],
        out_specs=[vmem, vmem, vmem, *[hbm] * chunks],
        scratch_shapes=[
            pltpu.VMEM((tall, width), f32),
            pltpu.VMEM((BUFFERS, size, width), bf16),
            pltpu.VMEM((shards, 1, capacity), i32),
            pltpu.VMEM((shards, 1, capacity), i32),
            pltpu.SMEM((shards, 1, capacity), i32),
            pltpu.SMEM((slates, 1, length), i32),
            pltpu.VMEM((max(PICK, *depths), width), f32),
            pltpu.VMEM((length, width), bf16),
            pltpu.VMEM((1, length), i32),
            *[pltpu.VMEM(block, bf16) for block in blocks],
            *[pltpu.VMEM(block, bf16) for block in blocks],
            *[pltpu.VMEM(w.shape, bf16) for w in weights],
            *[pltpu.VMEM(w.shape[::-1], bf16) for w in weights],
            *score_scratch(model, length, weights[3].shape[1]),
            pltpu.SemaphoreType.DMA((BUFFERS,)),
            pltpu.SemaphoreType.DMA((5,)),
            pltpu.SemaphoreType.DMA,
            pltpu.SemaphoreType.DMA,
            pltpu.SemaphoreType.DMA((2,)),
            pltpu.SemaphoreType.DMA((chunks,)),
            pltpu.SemaphoreType.DMA((chunks,)),
            pltpu.SemaphoreType.DMA((chunks,)),
        ],
        compiler_params=pltpu.CompilerParams(
            collective_id=0, has_side_effects=True, vmem_limit_bytes=67043328
        ),
        name="rank",
    )(owner, row_index, *gains, table, *weights)


def finish_kernel(flag_ref, ranked_ref, place_hbm, norm_hbm, final_hbm, score_hbm, *refs):
    raw_hbm, refs = refs[:5], refs[5:]
    chunks = len(refs) - 26
    kept_refs, out_ref, refs = refs[:chunks], refs[chunks], refs[chunks + 1 :]
    rows_ref, landed_ref, emb_ref, place_ref = refs[:4]
    gain_refs, raw, turned, scratch, sem = refs[4:7], refs[7:12], refs[12:17], refs[17:24], refs[24]
    slates, length = out_ref.shape
    model = norm_hbm.shape[1]
    redo = flag_ref[0, 0] > 0

    def fetch(source, target):
        copy = pltpu.make_async_copy(source, target, sem)
        copy.start()
        copy.wait()

    @pl.when(jnp.logical_not(redo))
    def _():
        for slate in range(slates):
            out_ref[slate : slate + 1, :] = ranked_ref[slate]

    @pl.when(redo)
    def _():
        fetch(place_hbm, place_ref)
        for source, target in zip((norm_hbm, final_hbm, score_hbm, *raw_hbm), (*gain_refs, *raw)):
            fetch(source, target)
        turn_weights(raw, turned)
        base = 0
        for kept in kept_refs:
            shards, depth, width = kept.shape
            fetch(kept, landed_ref.at[:, pl.ds(0, depth), :])

            @pl.loop(0, shards)
            def _(peer):
                start = pl.multiple_of(base + peer * depth, 16)
                rows_ref[pl.ds(start, depth), :] = landed_ref[peer, pl.ds(0, depth), :].astype(f32)

            base += shards * depth
        spread_gains(gain_refs, rows_ref, base)
        gain_of = lambda row, cols: widen(rows_ref, base, row, model, cols)

        @pl.loop(0, slates)
        def _(slate):
            @pl.loop(0, length // PICK)
            def _(block):
                for row in range(PICK):
                    index = block * PICK + row
                    emb_ref[pl.ds(index, 1), :] = rows_ref[pl.ds(place_ref[slate, 0, index], 1), :]

            result, low, high = score_slate(emb_ref[...].astype(bf16), turned, gain_of, scratch, True)
            out_ref[pl.ds(slate, 1), :] = result


def finish(flag, place, ranked, gains, weights, kept):
    slates, unused, length = ranked.shape
    model = gains[0].shape[1]
    shards, unused, width = kept[0].shape
    deepest = max(block.shape[1] for block in kept)
    capacity = sum(block.shape[1] for block in kept)
    vmem, hbm, smem = [pl.BlockSpec(memory_space=m) for m in (pltpu.VMEM, pltpu.HBM, pltpu.SMEM)]
    return pl.pallas_call(
        finish_kernel,
        out_shape=jax.ShapeDtypeStruct((slates, length), f32),
        in_specs=[smem, vmem, *[hbm] * (9 + len(kept))],
        out_specs=vmem,
        scratch_shapes=[
            pltpu.VMEM((shards * capacity + 4 * model, width), f32),
            pltpu.VMEM((shards, deepest, width), bf16),
            pltpu.VMEM((length, width), f32),
            pltpu.SMEM((slates, 1, length), i32),
            *[pltpu.VMEM(gain.shape, gain.dtype) for gain in gains],
            *[pltpu.VMEM(w.shape, bf16) for w in weights],
            *[pltpu.VMEM(w.shape[::-1], bf16) for w in weights],
            *score_scratch(model, length, weights[3].shape[1]),
            pltpu.SemaphoreType.DMA,
        ],
        compiler_params=pltpu.CompilerParams(vmem_limit_bytes=60 * 1024 * 1024),
        name="finish",
    )(flag, ranked, place, *gains, *weights, *kept)


def per_device(
    candidate_owner,
    candidate_row,
    item_table,
    w_in,
    w_qkv,
    w_out,
    w_up,
    w_down,
    norm_gains,
    final_gain,
    w_score,
):
    slates, length, unused = candidate_owner.shape
    shards = lax.axis_size(("gx", "gy"))
    capacity = max(16, 2 * slates * length // shards)
    owner = candidate_owner.reshape(slates, 1, length)
    gains = (norm_gains[0], final_gain[None, :], w_score)
    weights = (w_in, w_qkv[0], w_out[0], w_up[0], w_down[0])
    ranked, flag, place, *kept = rank(owner, candidate_row, gains, item_table, weights, capacity, shards)
    return finish(flag, place, ranked, gains, weights, kept)


def solution(mesh):
    return jax.shard_map(
        per_device,
        mesh=mesh,
        in_specs=(
            P(("gx", "gy"), None, None),
            P(("gx", "gy"), None),
            P(("gx", "gy"), None),
            P(),
            P(),
            P(),
            P(),
            P(),
            P(),
            P(),
            P(),
        ),
        out_specs=P(("gx", "gy"), None),
        check_vma=False,
    )
```
